32 devices in a mesh: dp: 2 (over x), ei: 4 (over z), eo: 4 (over y, core).
Axes of the slice: x: 2, y: 2, z: 4, core: 2. Of those that a mesh axis runs over, the one named last changes fastest.
Arguments:
- tokens: bfloat16 [8192, 2048], P(('dp', 'ei', 'eo')), parts along dimension 0
- expert_idx: int32 [8192, 4], P(('dp', 'ei', 'eo')), parts along dimension 0
- gates: float32 [8192, 4], P(('dp', 'ei', 'eo')), parts along dimension 0
- w_gate: bfloat16 [16, 2048, 1408], P(('ei', 'eo'))
- w_up: bfloat16 [16, 2048, 1408], P(('ei', 'eo'))
- w_down: bfloat16 [16, 1408, 2048], P(('ei', 'eo'))
- grad_out: bfloat16 [8192, 2048], P(('dp', 'ei', 'eo')), parts along dimension 0
Outputs:
- output 1: bfloat16 [8192, 2048], P(('dp', 'ei', 'eo')), parts along dimension 0
- output 2: bfloat16 [8192, 2048], P(('dp', 'ei', 'eo')), parts along dimension 0
- output 3: float32 [8192, 4], P(('dp', 'ei', 'eo')), parts along dimension 0
- output 4: bfloat16 [32, 2048, 1408], P(('dp', 'ei', 'eo')), parts along dimension 0
- output 5: bfloat16 [32, 2048, 1408], P(('dp', 'ei', 'eo')), parts along dimension 0
- output 6: bfloat16 [32, 1408, 2048], P(('dp', 'ei', 'eo')), parts along dimension 0
There are 2 independent parts. The reference program is written for one: setup_inputs(seed, part) draws one part's arguments, and reference() takes and returns one part's arrays. A program takes and returns all parts, laid end to end along the dimension named above; an argument that names none is the same for every part.
All inputs are finite; a program needn't handle non-finite values.
Results may differ from the reference program's by a relative error of at most 0.00495966.
Values are sent between devices in bfloat16 or wider.
A program may use at most 1 GiB of HBM per device.

```python
import jax
import jax.numpy as jnp
from jax import lax

GROUP_DEVS = 16
EXP_DEV = 1
TOK_DEV = 256
D_MODEL = 2048
D_FF = 1408
TOP_K = 4
NUM_EXPERTS = EXP_DEV * GROUP_DEVS
TOKENS = TOK_DEV * GROUP_DEVS
CAPACITY = min(TOK_DEV, TOK_DEV * TOP_K // (4 * EXP_DEV))


def draw_routes(route_key):
    hot_key, src_key = jax.random.split(route_key)
    hot_dev = jax.random.randint(hot_key, (), 0, GROUP_DEVS)
    expert_ids = jnp.arange(NUM_EXPERTS, dtype=jnp.int32)
    is_hot = expert_ids // EXP_DEV == hot_dev
    cold_n = NUM_EXPERTS - EXP_DEV
    rest_n = TOK_DEV * TOP_K - EXP_DEV * CAPACITY
    above_hot = (expert_ids >= (hot_dev + 1) * EXP_DEV).astype(jnp.int32)
    cold_pos = jnp.clip(expert_ids - EXP_DEV * above_hot, 0, cold_n - 1)
    positions = jnp.arange(TOK_DEV * TOP_K, dtype=jnp.int32)

    def one_source(source_key):
        perm_key, row_key, rot_key = jax.random.split(source_key, 3)
        cold_rank = jax.random.permutation(perm_key, cold_n)
        cold_count = rest_n // cold_n + (cold_rank[cold_pos] < rest_n % cold_n).astype(jnp.int32)
        counts = jnp.where(is_hot, CAPACITY, cold_count).astype(jnp.int32)
        listing = jnp.searchsorted(jnp.cumsum(counts), positions, side='right').astype(jnp.int32)
        route_table = listing.reshape(TOP_K, TOK_DEV).T[jax.random.permutation(row_key, TOK_DEV)]
        row_shift = jax.random.randint(rot_key, (TOK_DEV, 1), 0, TOP_K)
        col_order = (jnp.arange(TOP_K)[None, :] + row_shift) % TOP_K
        return jnp.take_along_axis(route_table, col_order, axis=1)

    source_keys = jax.random.split(src_key, GROUP_DEVS)
    return jax.vmap(one_source)(source_keys).reshape(TOKENS, TOP_K).astype(jnp.int32)


def setup_inputs(seed: int = 0, part: int = 0) -> dict:
    part_key = jax.random.fold_in(jax.random.key(seed), part)
    tok_key, route_key, gate_key, dy_key = jax.random.split(part_key, 4)
    gate_w_key, up_w_key, down_w_key = jax.random.split(jax.random.key(seed + 1), 3)
    tokens = jax.random.normal(tok_key, (TOKENS, D_MODEL), jnp.float32).astype(jnp.bfloat16)
    expert_idx = draw_routes(route_key)
    gates = jax.random.uniform(gate_key, (TOKENS, TOP_K), jnp.float32, 0.05, 0.3)
    w_gate = (jax.random.normal(gate_w_key, (NUM_EXPERTS, D_MODEL, D_FF), jnp.float32) * D_MODEL ** -0.5).astype(jnp.bfloat16)
    w_up = (jax.random.normal(up_w_key, (NUM_EXPERTS, D_MODEL, D_FF), jnp.float32) * D_MODEL ** -0.5).astype(jnp.bfloat16)
    w_down = (jax.random.normal(down_w_key, (NUM_EXPERTS, D_FF, D_MODEL), jnp.float32) * D_FF ** -0.5).astype(jnp.bfloat16)
    grad_out = jax.random.normal(dy_key, (TOKENS, D_MODEL), jnp.float32).astype(jnp.bfloat16)
    return {'tokens': tokens, 'expert_idx': expert_idx, 'gates': gates, 'w_gate': w_gate, 'w_up': w_up, 'w_down': w_down, 'grad_out': grad_out}


def reference(tokens, expert_idx, gates, w_gate, w_up, w_down, grad_out):
    n_assign = TOKENS * TOP_K
    expert_cap = GROUP_DEVS * CAPACITY
    flat_e = expert_idx.reshape(-1)
    sort_order = jnp.argsort(flat_e, stable=True).astype(jnp.int32)
    sorted_e = flat_e[sort_order]
    counts = jnp.zeros((NUM_EXPERTS,), jnp.int32).at[flat_e].add(1)
    starts = jnp.cumsum(counts) - counts
    slot_rank = jnp.arange(n_assign, dtype=jnp.int32) - starts[sorted_e]
    filler = jnp.full((NUM_EXPERTS * expert_cap,), n_assign, jnp.int32).at[sorted_e * expert_cap + slot_rank].set(sort_order)
    filler = filler.reshape(NUM_EXPERTS, expert_cap)
    tok_pad = jnp.concatenate([tokens, jnp.zeros((1, D_MODEL), tokens.dtype)])
    dy_pad = jnp.concatenate([grad_out, jnp.zeros((1, D_MODEL), grad_out.dtype)])
    gate_pad = jnp.concatenate([gates.reshape(-1), jnp.zeros((1,), jnp.float32)])

    def one_expert(acc_state, expert_in):
        out_acc, dx_acc, dg_acc = acc_state
        wg_e, wu_e, wd_e, assign = expert_in
        tok_ids = assign // TOP_K
        x_rows = tok_pad[tok_ids]
        g_rows = gate_pad[assign]
        dy_rows = dy_pad[tok_ids]
        h_gate = jnp.dot(x_rows, wg_e, preferred_element_type=jnp.float32)
        h_up = jnp.dot(x_rows, wu_e, preferred_element_type=jnp.float32)
        sig_gate = jax.nn.sigmoid(h_gate)
        hidden = (h_gate * sig_gate * h_up).astype(jnp.bfloat16)
        y_rows = jnp.dot(hidden, wd_e, preferred_element_type=jnp.float32).astype(jnp.bfloat16)
        dg_rows = jnp.sum(dy_rows.astype(jnp.float32) * y_rows.astype(jnp.float32), axis=1)
        u_rows = (g_rows[:, None] * dy_rows.astype(jnp.float32)).astype(jnp.bfloat16)
        d_hidden = jnp.dot(u_rows, wd_e.T, preferred_element_type=jnp.float32)
        d_up = (d_hidden * h_gate * sig_gate).astype(jnp.bfloat16)
        d_gate = (d_hidden * h_up * sig_gate * (1.0 + h_gate * (1.0 - sig_gate))).astype(jnp.bfloat16)
        dx_rows = (jnp.dot(d_gate, wg_e.T, preferred_element_type=jnp.float32) + jnp.dot(d_up, wu_e.T, preferred_element_type=jnp.float32)).astype(jnp.bfloat16)
        dw_gate = jnp.dot(x_rows.T, d_gate, preferred_element_type=jnp.float32).astype(jnp.bfloat16)
        dw_up = jnp.dot(x_rows.T, d_up, preferred_element_type=jnp.float32).astype(jnp.bfloat16)
        dw_down = jnp.dot(hidden.T, u_rows, preferred_element_type=jnp.float32).astype(jnp.bfloat16)
        out_acc = out_acc.at[tok_ids].add(g_rows[:, None] * y_rows.astype(jnp.float32))
        dx_acc = dx_acc.at[tok_ids].add(dx_rows.astype(jnp.float32))
        dg_acc = dg_acc.at[assign].add(dg_rows)
        return (out_acc, dx_acc, dg_acc), (dw_gate, dw_up, dw_down)

    zero_state = (jnp.zeros((TOKENS + 1, D_MODEL), jnp.float32), jnp.zeros((TOKENS + 1, D_MODEL), jnp.float32), jnp.zeros((n_assign + 1,), jnp.float32))
    final_state, weight_grads = lax.scan(one_expert, zero_state, (w_gate, w_up, w_down, filler))
    out_acc, dx_acc, dg_acc = final_state
    dw_gate, dw_up, dw_down = weight_grads
    layer_out = out_acc[:TOKENS].astype(jnp.bfloat16)
    grad_tokens = dx_acc[:TOKENS].astype(jnp.bfloat16)
    grad_gates = dg_acc[:n_assign].reshape(TOKENS, TOP_K)
    return (layer_out, grad_tokens, grad_gates, dw_gate, dw_up, dw_down)
```

```python
import jax
import jax.numpy as jnp
from jax import lax
from jax.sharding import PartitionSpec as P


def solution(mesh):
    axes = ('ei', 'eo')
    eo_size = mesh.shape['eo']
    tok_spec = P(('dp', 'ei', 'eo'))
    exp_spec = P(('ei', 'eo'))

    def device_step(tok_loc, idx_loc, gate_loc, w_gate, w_up, w_down, dy_loc):
        me = lax.axis_index('ei') * eo_size + lax.axis_index('eo')
        w_gate, w_up, w_down = w_gate[0], w_up[0], w_down[0]
        x = lax.all_gather(tok_loc, axes, axis=0, tiled=True)
        dy = lax.all_gather(dy_loc, axes, axis=0, tiled=True)
        idx = lax.all_gather(idx_loc, axes, axis=0, tiled=True)
        gates = lax.all_gather(gate_loc, axes, axis=0, tiled=True)
        hit = idx == me
        routed = jnp.any(hit, axis=1, keepdims=True)
        gate = jnp.sum(jnp.where(hit, gates, 0.0), axis=1, keepdims=True)
        f32 = jnp.float32
        a = jnp.where(routed, jnp.dot(x, w_gate, preferred_element_type=f32), 0.0)
        b = jnp.where(routed, jnp.dot(x, w_up, preferred_element_type=f32), 0.0)
        s = jax.nn.sigmoid(a)
        h = (a * s * b).astype(jnp.bfloat16)
        o = jnp.dot(h, w_down, preferred_element_type=f32).astype(jnp.bfloat16).astype(f32)
        layer_out = lax.psum_scatter(gate * o, axes, scatter_dimension=0, tiled=True).astype(jnp.bfloat16)
        dyf = dy.astype(f32)
        dg_tok = jnp.sum(dyf * o, axis=1)
        dg_all = lax.all_gather(dg_tok.reshape(16, -1)[:, None, :], axes, axis=1, tiled=True)
        mine = lax.dynamic_index_in_dim(dg_all, me, 0, keepdims=False)
        grad_gates = jnp.take_along_axis(mine.T, idx_loc, axis=1)
        u = (gate * dyf).astype(jnp.bfloat16)
        q = lax.dot_general(u, w_down, (((1,), (1,)), ((), ())), preferred_element_type=f32)
        du = (q * a * s).astype(jnp.bfloat16)
        dg = (q * b * s * (1.0 + a * (1.0 - s))).astype(jnp.bfloat16)
        nt = (((1,), (1,)), ((), ()))
        tn = (((0,), (0,)), ((), ()))
        dx = (lax.dot_general(dg, w_gate, nt, preferred_element_type=f32) + lax.dot_general(du, w_up, nt, preferred_element_type=f32)).astype(jnp.bfloat16).astype(f32)
        grad_tokens = lax.psum_scatter(dx, axes, scatter_dimension=0, tiled=True).astype(jnp.bfloat16)
        gwg = lax.dot_general(x, dg, tn, preferred_element_type=f32).astype(jnp.bfloat16)
        gwu = lax.dot_general(x, du, tn, preferred_element_type=f32).astype(jnp.bfloat16)
        gwd = lax.dot_general(h, u, tn, preferred_element_type=f32).astype(jnp.bfloat16)
        return layer_out, grad_tokens, grad_gates, gwg[None], gwu[None], gwd[None]

    return jax.shard_map(device_step, mesh=mesh, in_specs=(tok_spec, tok_spec, tok_spec, exp_spec, exp_spec, exp_spec, tok_spec), out_specs=(tok_spec, tok_spec, tok_spec, tok_spec, tok_spec, tok_spec), check_vma=False)
```

```python
import jax
import jax.numpy as jnp
from jax import lax
from jax.sharding import PartitionSpec as P


def ring_tables(ei_size, eo_size):
    chips_y = eo_size // 2
    walk = [(z, 0) for z in range(ei_size)] + [(z, 1) for z in reversed(range(ei_size))]
    assert chips_y == 2
    return [[z * eo_size + y * 2 + core for core in range(2)] for z, y in walk]


def solution(mesh):
    axes = ('ei', 'eo')
    ei_size, eo_size = mesh.shape['ei'], mesh.shape['eo']
    table = ring_tables(ei_size, eo_size)
    ring = len(table)
    half = ring // 2
    group = ei_size * eo_size
    pairs = lambda step: [(table[p][c], table[(p + step) % ring][c]) for p in range(ring) for c in range(2)]
    cw_perm, ccw_perm = pairs(1), pairs(-1)
    swap_perm = [(table[p][c], table[p][1 - c]) for p in range(ring) for c in range(2)]
    rel_order = [None] * group
    for p in range(ring):
        for c in range(2):
            rel_order[table[p][c]] = [table[(p + r) % ring][c ^ k] for r in range(ring) for k in range(2)]
    tok_spec = P(('dp', 'ei', 'eo'))
    exp_spec = P(('ei', 'eo'))
    f32 = jnp.float32
    bf16 = jnp.bfloat16
    nt = (((1,), (1,)), ((), ()))
    tn = (((0,), (0,)), ((), ()))
    chunks = [(0,)] + [(ring - k, k) for k in range(1, half)] + [(half,)]

    def cw(v):
        return lax.ppermute(v, axes, cw_perm)

    def ccw(v):
        return lax.ppermute(v, axes, ccw_perm)

    def swap(v):
        return lax.ppermute(v, axes, swap_perm)

    def gather_rings(*owns):
        width = owns[0].shape[1] // 2
        got = [[own] + [None] * (ring - 1) for own in owns]
        for k in range(1, half):
            for blocks in got:
                blocks[ring - k] = cw(blocks[(ring - k + 1) % ring])
                blocks[k] = ccw(blocks[k - 1])
        for blocks in got:
            left = cw(blocks[half + 1][:, :width])
            right = ccw(blocks[half - 1][:, width:])
            blocks[half] = jnp.concatenate([left, right], axis=1)
        return [[(v, swap(v)) for v in blocks] for blocks in got]

    def scatter_step(s, acc, term):
        if s == 0:
            return term(ring - 1, 0), term(1, 1)
        left = cw(acc[0])
        right = ccw(acc[1])
        return left + term(ring - 1 - s, 0), right + term((1 + s) % ring, 1)

    def device_step(tok_loc, idx_loc, gate_loc, w_gate, w_up, w_down, dy_loc):
        me = lax.axis_index('ei') * eo_size + lax.axis_index('eo')
        tok_dev, top_k = idx_loc.shape
        d_model = tok_loc.shape[1]
        width = d_model // 2
        w_gate, w_up, w_down = w_gate[0], w_up[0], w_down[0]

        meta = jnp.concatenate([idx_loc.astype(f32), gate_loc], axis=1)
        meta = lax.all_gather(meta, axes, axis=0, tiled=True)
        meta, tok_loc, dy_loc = lax.optimization_barrier((meta, tok_loc, dy_loc))
        meta = meta.reshape(group, tok_dev, 2 * top_k)
        x_blk, dy_blk = gather_rings(tok_loc, dy_loc)
        meta = meta[jnp.array(rel_order, jnp.int32)[me]]
        ids, gates = meta[:, :, :top_k].astype(jnp.int32), meta[:, :, top_k:]

        def gate_of(expert):
            hit = ids == expert
            return jnp.any(hit, axis=2), jnp.sum(jnp.where(hit, gates, 0.0), axis=2)

        routed, gate = gate_of(me)
        _, gate_mate = gate_of(me ^ 1)

        saved = []
        y_of, dx_of, y_mate, dx_mate = {}, {}, {}, {}

        def y_term(r, side):
            cols = slice(side * width, (side + 1) * width)
            return gate[r * 2][:, None] * y_of[r, 0][:, cols].astype(f32) + gate_mate[r * 2][:, None] * y_mate[r][:, cols].astype(f32)

        def dx_term(r, side):
            cols = slice(side * width, (side + 1) * width)
            return dx_of[r, 0][:, cols].astype(f32) + dx_mate[r][:, cols].astype(f32)

        def dot_term(r):
            dyf = dy_blk[r][0].astype(f32)
            own = jnp.sum(dyf * y_of[r, 0].astype(f32), axis=1)
            mate = jnp.sum(dyf * y_mate[r].astype(f32), axis=1)
            return jnp.where(ids[r * 2] == me, own[:, None], 0.0).T + jnp.where(ids[r * 2] == (me ^ 1), mate[:, None], 0.0).T

        y_acc = dx_acc = dot_acc = None

        def advance(s):
            nonlocal y_acc, dx_acc, dot_acc
            dot_acc = dot_term(ring - 1 - s) if s == 0 else cw(dot_acc) + dot_term(ring - 1 - s)
            y_acc = scatter_step(s, y_acc, y_term)
            dx_acc = scatter_step(s, dx_acc, dx_term)
            if s < ring - 1:
                y_acc, dx_acc, dot_acc = lax.optimization_barrier((y_acc, dx_acc, dot_acc))

        for n, offs in enumerate(chunks):
            names = [(r, k) for r in offs for k in range(2)]
            x = jnp.concatenate([x_blk[r][k] for r, k in names])
            dy = jnp.concatenate([dy_blk[r][k] for r, k in names])
            pick = lambda v: jnp.concatenate([v[r * 2 + k] for r, k in names])[:, None]
            on, g = pick(routed), pick(gate)
            a = jnp.where(on, jnp.dot(x, w_gate, preferred_element_type=f32), 0.0)
            b = jnp.where(on, jnp.dot(x, w_up, preferred_element_type=f32), 0.0)
            s = jax.nn.sigmoid(a)
            h = (a * s * b).astype(bf16)
            o = jnp.dot(h, w_down, preferred_element_type=f32).astype(bf16)
            u = (g * dy.astype(f32)).astype(bf16)
            q = lax.dot_general(u, w_down, nt, preferred_element_type=f32)
            du = (q * a * s).astype(bf16)
            dg = (q * b * s * (1.0 + a * (1.0 - s))).astype(bf16)
            dx = (lax.dot_general(dg, w_gate, nt, preferred_element_type=f32) + lax.dot_general(du, w_up, nt, preferred_element_type=f32)).astype(bf16)
            saved.append((h, u, dg, du))
            for i, (r, k) in enumerate(names):
                rows = slice(i * tok_dev, (i + 1) * tok_dev)
                y_of[r, k], dx_of[r, k] = o[rows], dx[rows]
            for r in offs:
                y_mate[r], dx_mate[r] = swap(y_of[r, 1]), swap(dx_of[r, 1])
            if n >= 1:
                advance(n - 1)

        for s in range(len(chunks) - 1, ring):
            advance(s)
        layer_out = jnp.concatenate(y_acc, axis=1).astype(bf16)
        grad_tokens = jnp.concatenate(dx_acc, axis=1).astype(bf16)
        grad_gates = dot_acc.T

        x_cat = jnp.concatenate([x_blk[r][k] for offs in chunks for r in offs for k in range(2)])
        h, u, dg, du = (jnp.concatenate(v) for v in zip(*saved))
        gwg = lax.dot_general(x_cat, dg, tn, preferred_element_type=f32).astype(bf16)
        gwu = lax.dot_general(x_cat, du, tn, preferred_element_type=f32).astype(bf16)
        gwd = lax.dot_general(h, u, tn, preferred_element_type=f32).astype(bf16)
        return layer_out, grad_tokens, grad_gates, gwg[None], gwu[None], gwd[None]

    return jax.shard_map(device_step, mesh=mesh, in_specs=(tok_spec, tok_spec, tok_spec, exp_spec, exp_spec, exp_spec, tok_spec), out_specs=(tok_spec, tok_spec, tok_spec, tok_spec, tok_spec, tok_spec), check_vma=False)
```

```python
import jax
import jax.numpy as jnp
from jax import lax
from jax.sharding import PartitionSpec as P


def ring_tables(ei_size, eo_size):
    chips_y = eo_size // 2
    walk = [(z, 0) for z in range(ei_size)] + [(z, 1) for z in reversed(range(ei_size))]
    assert chips_y == 2
    return [[z * eo_size + y * 2 + core for core in range(2)] for z, y in walk]


def solution(mesh):
    axes = ('ei', 'eo')
    ei_size, eo_size = mesh.shape['ei'], mesh.shape['eo']
    table = ring_tables(ei_size, eo_size)
    ring = len(table)
    half = ring // 2
    pairs = lambda step: [(table[p][c], table[(p + step) % ring][c]) for p in range(ring) for c in range(2)]
    cw_perm, ccw_perm = pairs(1), pairs(-1)
    swap_perm = [(table[p][c], table[p][1 - c]) for p in range(ring) for c in range(2)]
    tok_spec = P(('dp', 'ei', 'eo'))
    exp_spec = P(('ei', 'eo'))
    f32 = jnp.float32
    bf16 = jnp.bfloat16
    nt = (((1,), (1,)), ((), ()))
    tn = (((0,), (0,)), ((), ()))
    chunks = [(ring - k, k) for k in range(1, half)] + [(half,), (0,)]

    def cw(v):
        return lax.ppermute(v, axes, cw_perm)

    def ccw(v):
        return lax.ppermute(v, axes, ccw_perm)

    def swap(v):
        return lax.ppermute(v, axes, swap_perm)

    def direct(v, r, k):
        perm = [(table[(p + r) % ring][c ^ k], table[p][c]) for p in range(ring) for c in range(2)]
        return lax.ppermute(v, axes, perm) if r or k else v

    def gather_rings(*owns):
        got = [[own] + [None] * (ring - 1) for own in owns]
        for k in range(1, half):
            for blocks in got:
                blocks[ring - k] = cw(blocks[(ring - k + 1) % ring])
                blocks[k] = ccw(blocks[k - 1])
        for blocks in got:
            width = blocks[0].shape[1] // 2
            left = cw(blocks[half + 1][:, :width])
            right = ccw(blocks[half - 1][:, width:])
            blocks[half] = jnp.concatenate([left, right], axis=1)
        return [[(v, swap(v)) for v in blocks] for blocks in got]

    def scatter_step(s, acc, term):
        if s == 0:
            return term(ring - 1, 0), term(1, 1)
        left = cw(acc[0])
        right = ccw(acc[1])
        return left + term(ring - 1 - s, 0), right + term((1 + s) % ring, 1)

    def device_step(tok_loc, idx_loc, gate_loc, w_gate, w_up, w_down, dy_loc):
        me = lax.axis_index('ei') * eo_size + lax.axis_index('eo')
        tok_dev, top_k = idx_loc.shape
        d_model = tok_loc.shape[1]
        width = d_model // 2
        w_gate, w_up, w_down = w_gate[0], w_up[0], w_down[0]

        meta_loc = jnp.concatenate([idx_loc.astype(f32), gate_loc], axis=1).T
        meta_blk = [[direct(meta_loc, r, k) for k in range(2)] for r in range(ring)]
        x_blk, dy_blk = gather_rings(tok_loc, dy_loc)

        def gate_of(meta, expert):
            hit = meta[:top_k].astype(jnp.int32) == expert
            return hit, jnp.sum(jnp.where(hit, meta[top_k:], 0.0), axis=0)[:, None]

        saved = []
        y_of, dx_of, y_mate, dx_mate = {}, {}, {}, {}

        def y_term(r, side):
            cols = slice(side * width, (side + 1) * width)
            return gate_of(meta_blk[r][0], me)[1] * y_of[r][:, cols].astype(f32) + gate_of(meta_blk[r][0], me ^ 1)[1] * y_mate[r][:, cols].astype(f32)

        def dx_term(r, side):
            cols = slice(side * width, (side + 1) * width)
            return dx_of[r][:, cols].astype(f32) + dx_mate[r][:, cols].astype(f32)

        def dot_term(r):
            dyf = dy_blk[r][0].astype(f32)
            own = jnp.sum(dyf * y_of[r].astype(f32), axis=1)
            mate = jnp.sum(dyf * y_mate[r].astype(f32), axis=1)
            hit, hit_mate = (gate_of(meta_blk[r][0], expert)[0] for expert in (me, me ^ 1))
            return jnp.where(hit, own[None, :], 0.0) + jnp.where(hit_mate, mate[None, :], 0.0)

        y_acc = dx_acc = dot_acc = None

        def advance(s):
            nonlocal y_acc, dx_acc, dot_acc
            dot_acc = dot_term(ring - 1 - s) if s == 0 else cw(dot_acc) + dot_term(ring - 1 - s)
            y_acc = scatter_step(s, y_acc, y_term)
            dx_acc = scatter_step(s, dx_acc, dx_term)
            if s < ring - 1:
                y_acc, dx_acc, dot_acc = lax.optimization_barrier((y_acc, dx_acc, dot_acc))

        for n, offs in enumerate(chunks):
            names = [(r, k) for k in range(2) for r in offs]
            x = jnp.concatenate([x_blk[r][k] for r, k in names])
            dy = jnp.concatenate([dy_blk[r][k] for r, k in names])
            meta = jnp.concatenate([meta_blk[r][k] for r, k in names], axis=1)
            hit, g = gate_of(meta, me)
            on = jnp.any(hit, axis=0)[:, None]
            a = jnp.where(on, jnp.dot(x, w_gate, preferred_element_type=f32), 0.0)
            b = jnp.where(on, jnp.dot(x, w_up, preferred_element_type=f32), 0.0)
            s = jax.nn.sigmoid(a)
            h = (a * s * b).astype(bf16)
            o = jnp.dot(h, w_down, preferred_element_type=f32).astype(bf16)
            u = (g * dy.astype(f32)).astype(bf16)
            q = lax.dot_general(u, w_down, nt, preferred_element_type=f32)
            du = (q * a * s).astype(bf16)
            dg = (q * b * s * (1.0 + a * (1.0 - s))).astype(bf16)
            dx = (lax.dot_general(dg, w_gate, nt, preferred_element_type=f32) + lax.dot_general(du, w_up, nt, preferred_element_type=f32)).astype(bf16)
            saved.append((h, u, dg, du))
            split = len(offs) * tok_dev
            o_mate, dxs_mate = swap(o[split:]), swap(dx[split:])
            for i, r in enumerate(offs):
                rows = slice(i * tok_dev, (i + 1) * tok_dev)
                y_of[r], dx_of[r] = o[rows], dx[rows]
                y_mate[r], dx_mate[r] = o_mate[rows], dxs_mate[rows]
            if n < half:
                advance(n)

        for s in range(half, ring):
            advance(s)
        layer_out = jnp.concatenate(y_acc, axis=1).astype(bf16)
        grad_tokens = jnp.concatenate(dx_acc, axis=1).astype(bf16)
        grad_gates = dot_acc.T

        x_cat = jnp.concatenate([x_blk[r][k] for offs in chunks for k in range(2) for r in offs])
        h, u, dg, du = (jnp.concatenate(v) for v in zip(*saved))
        gwg = lax.dot_general(x_cat, dg, tn, preferred_element_type=f32).astype(bf16)
        gwu = lax.dot_general(x_cat, du, tn, preferred_element_type=f32).astype(bf16)
        gwd = lax.dot_general(h, u, tn, preferred_element_type=f32).astype(bf16)
        return layer_out, grad_tokens, grad_gates, gwg[None], gwu[None], gwd[None]

    return jax.shard_map(device_step, mesh=mesh, in_specs=(tok_spec, tok_spec, tok_spec, exp_spec, exp_spec, exp_spec, tok_spec), out_specs=(tok_spec, tok_spec, tok_spec, tok_spec, tok_spec, tok_spec), check_vma=False)
```

```python
import jax
import jax.numpy as jnp
from jax import lax
from jax.sharding import PartitionSpec as P


def ring_tables(ei_size, eo_size):
    chips_y = eo_size // 2
    walk = [(z, 0) for z in range(ei_size)] + [(z, 1) for z in reversed(range(ei_size))]
    assert chips_y == 2
    return [[z * eo_size + y * 2 + core for core in range(2)] for z, y in walk]


def solution(mesh):
    axes = ('ei', 'eo')
    ei_size, eo_size = mesh.shape['ei'], mesh.shape['eo']
    table = ring_tables(ei_size, eo_size)
    ring = len(table)
    half = ring // 2
    group = ei_size * eo_size
    pairs = lambda step: [(table[p][c], table[(p + step) % ring][c]) for p in range(ring) for c in range(2)]
    cw_perm, ccw_perm = pairs(1), pairs(-1)
    swap_perm = [(table[p][c], table[p][1 - c]) for p in range(ring) for c in range(2)]
    rel_order = [None] * group
    for p in range(ring):
        for c in range(2):
            rel_order[table[p][c]] = [table[(p + r) % ring][c ^ k] for r in range(ring) for k in range(2)]
    tok_spec = P(('dp', 'ei', 'eo'))
    exp_spec = P(('ei', 'eo'))
    f32 = jnp.float32
    bf16 = jnp.bfloat16
    nt = (((1,), (1,)), ((), ()))
    tn = (((0,), (0,)), ((), ()))
    chunks = [(0,)] + [(ring - k, k) for k in range(1, half)] + [(half,)]

    def cw(v):
        return lax.ppermute(v, axes, cw_perm)

    def ccw(v):
        return lax.ppermute(v, axes, ccw_perm)

    def swap(v):
        return lax.ppermute(v, axes, swap_perm)

    def gather_rings(*owns):
        width = owns[0].shape[1] // 2
        got = [[own] + [None] * (ring - 1) for own in owns]

        for k in range(1, half):
            for blocks in got:
                blocks[ring - k] = cw(blocks[(ring - k + 1) % ring])
                blocks[k] = ccw(blocks[k - 1])
        for blocks in got:
            left = cw(blocks[half + 1][:, :width])
            right = ccw(blocks[half - 1][:, width:])
            blocks[half] = jnp.concatenate([left, right], axis=1)
        return [[(v, swap(v)) for v in blocks] for blocks in got]

    def scatter_step(s, acc, term):
        if s == 0:
            return term(ring - 1, 0), term(1, 1)
        left = cw(acc[0])
        right = ccw(acc[1])
        return left + term(ring - 1 - s, 0), right + term((1 + s) % ring, 1)

    def device_step(tok_loc, idx_loc, gate_loc, w_gate, w_up, w_down, dy_loc):
        me = lax.axis_index('ei') * eo_size + lax.axis_index('eo')
        tok_dev, top_k = idx_loc.shape
        d_model = tok_loc.shape[1]
        width = d_model // 2
        w_gate, w_up, w_down = w_gate[0], w_up[0], w_down[0]

        meta = jnp.concatenate([idx_loc.astype(f32), gate_loc], axis=1)
        meta = lax.all_gather(meta, axes, axis=0, tiled=True)
        meta, tok_loc, dy_loc = lax.optimization_barrier((meta, tok_loc, dy_loc))
        meta = meta.reshape(group, tok_dev, 2 * top_k)
        x_blk, dy_blk = gather_rings(tok_loc, dy_loc)
        meta = meta[jnp.array(rel_order, jnp.int32)[me]]
        ids, gates = meta[:, :, :top_k].astype(jnp.int32), meta[:, :, top_k:]

        def gate_of(expert):
            hit = ids == expert
            return jnp.any(hit, axis=2), jnp.sum(jnp.where(hit, gates, 0.0), axis=2)

        routed, gate = gate_of(me)
        _, gate_mate = gate_of(me ^ 1)

        saved = []
        y_of, dx_of, y_mate, dx_mate = {}, {}, {}, {}

        def y_term(r, side):
            cols = slice(side * width, (side + 1) * width)
            return gate[r * 2][:, None] * y_of[r][:, cols].astype(f32) + gate_mate[r * 2][:, None] * y_mate[r][:, cols].astype(f32)

        def dx_term(r, side):
            cols = slice(side * width, (side + 1) * width)
            return dx_of[r][:, cols].astype(f32) + dx_mate[r][:, cols].astype(f32)

        def dot_term(r):
            dyf = dy_blk[r][0].astype(f32)
            own = jnp.sum(dyf * y_of[r].astype(f32), axis=1)
            mate = jnp.sum(dyf * y_mate[r].astype(f32), axis=1)
            return jnp.where(ids[r * 2] == me, own[:, None], 0.0).T + jnp.where(ids[r * 2] == (me ^ 1), mate[:, None], 0.0).T

        y_acc = dx_acc = dot_acc = None

        def advance(s):
            nonlocal y_acc, dx_acc, dot_acc
            dot_acc = dot_term(ring - 1 - s) if s == 0 else cw(dot_acc) + dot_term(ring - 1 - s)
            y_acc = scatter_step(s, y_acc, y_term)
            dx_acc = scatter_step(s, dx_acc, dx_term)
            if s < ring - 1:
                y_acc, dx_acc, dot_acc = lax.optimization_barrier((y_acc, dx_acc, dot_acc))

        for n, offs in enumerate(chunks):
            names = [(r, k) for k in range(2) for r in offs]
            x = jnp.concatenate([x_blk[r][k] for r, k in names])
            dy = jnp.concatenate([dy_blk[r][k] for r, k in names])
            pick = lambda v: jnp.concatenate([v[r * 2 + k] for r, k in names])[:, None]
            on, g = pick(routed), pick(gate)
            a = jnp.where(on, jnp.dot(x, w_gate, preferred_element_type=f32), 0.0)
            b = jnp.where(on, jnp.dot(x, w_up, preferred_element_type=f32), 0.0)
            s = jax.nn.sigmoid(a)
            h = (a * s * b).astype(bf16)
            o = jnp.dot(h, w_down, preferred_element_type=f32).astype(bf16)
            u = (g * dy.astype(f32)).astype(bf16)
            q = lax.dot_general(u, w_down, nt, preferred_element_type=f32)
            du = (q * a * s).astype(bf16)
            dg = (q * b * s * (1.0 + a * (1.0 - s))).astype(bf16)
            dx = (lax.dot_general(dg, w_gate, nt, preferred_element_type=f32) + lax.dot_general(du, w_up, nt, preferred_element_type=f32)).astype(bf16)
            saved.append((h, u, dg, du))
            split = len(offs) * tok_dev
            o_mate, dxs_mate = swap(o[split:]), swap(dx[split:])
            for i, r in enumerate(offs):
                rows = slice(i * tok_dev, (i + 1) * tok_dev)
                y_of[r], dx_of[r] = o[rows], dx[rows]
                y_mate[r], dx_mate[r] = o_mate[rows], dxs_mate[rows]
            if n >= 1:
                advance(n - 1)

        for s in range(len(chunks) - 1, ring):
            advance(s)
        layer_out = jnp.concatenate(y_acc, axis=1).astype(bf16)
        grad_tokens = jnp.concatenate(dx_acc, axis=1).astype(bf16)
        grad_gates = dot_acc.T

        x_cat = jnp.concatenate([x_blk[r][k] for offs in chunks for k in range(2) for r in offs])
        h, u, dg, du = (jnp.concatenate(v) for v in zip(*saved))
        gwg = lax.dot_general(x_cat, dg, tn, preferred_element_type=f32).astype(bf16)
        gwu = lax.dot_general(x_cat, du, tn, preferred_element_type=f32).astype(bf16)
        gwd = lax.dot_general(h, u, tn, preferred_element_type=f32).astype(bf16)
        return layer_out, grad_tokens, grad_gates, gwg[None], gwu[None], gwd[None]

    return jax.shard_map(device_step, mesh=mesh, in_specs=(tok_spec, tok_spec, tok_spec, exp_spec, exp_spec, exp_spec, tok_spec), out_specs=(tok_spec, tok_spec, tok_spec, tok_spec, tok_spec, tok_spec), check_vma=False)
```
